128 devices in a mesh: dp: 16 (over x_hi, z, core), tensor: 8 (over y, x_lo).
Axes of the slice: x: 4 (x_hi: 2, x_lo: 2; x = x_hi * 2 + x_lo), y: 4, z: 4, core: 2. Of those that a mesh axis runs over, the one named last changes fastest.
Arguments:
- latents: bfloat16 [176, 256, 640], P('dp', 'tensor'), may hold values from -6 to 6
- cotangent: bfloat16 [176, 256, 640], P('dp', 'tensor'), may hold values from -6 to 6
- trunc_steps: int32 [16], replicated, may hold values from 30 to 40, as said below
- timesteps: int32 [176], replicated, may hold values from 100 to 900
- tile_map: int32 [176], replicated, may hold values from 0 to 175, as said below
- gain: float32 [640], replicated, may hold values from 0.5 to 1.5
- w_value: bfloat16 [640, 2560], P(None, 'tensor'), may hold values from -0.25 to 0.25
- w_gate: bfloat16 [640, 2560], P(None, 'tensor'), may hold values from -0.25 to 0.25
- w_out: bfloat16 [640, 2560], P(None, 'tensor'), may hold values from -0.125 to 0.125
Outputs:
- placed_grad: bfloat16 [176, 256, 640], P('dp', 'tensor')
- grad_value: float32 [640, 2560], P('dp', 'tensor')
- grad_gate: float32 [640, 2560], P('dp', 'tensor')
- grad_out_proj: float32 [640, 2560], P('dp', 'tensor')
- grad_gain: float32 [640], replicated
The draws below stay inside these ranges and needn't reach their ends.
Inputs may be any that keep to these rules, and one draw needn't show every extreme that they name: trunc_steps lies in 30 to 40, so a prompt has 1 to 11 live slots, its lowest ones. tile_map is a permutation of 0 to 175. Output slots g * 11 to g * 11 + 10 form group g; the live items go to the lowest slots of the groups, and each group receives the floor or the ceiling of (number of live items) / 16 of them.
All inputs are finite; a program needn't handle non-finite values.
Results may differ from the reference program's by a relative error of at most 0.0068.
Values may be sent and summed in bfloat16 or wider, within the bound.
A program may use at most 64 MiB of HBM per device.

```python
import jax
import jax.numpy as jnp
from jax import lax

C = 640
FI = 2560
ROWS = 256
SLOTS = 11
PROMPTS = 16
ITEMS = 176


def chain_plan(key):
    steps = jax.random.randint(jax.random.fold_in(key, 11), (PROMPTS,), 30, 41).astype(jnp.int32)
    item_ids = jnp.arange(ITEMS, dtype=jnp.int32)
    live = (item_ids % SLOTS < jnp.repeat(steps, SLOTS) - 29).astype(jnp.int32)
    shuffled = jax.random.permutation(jax.random.fold_in(key, 12), ITEMS).astype(jnp.int32)
    ranking = (1 - live) * ITEMS + shuffled
    ordering = jnp.argsort(ranking, stable=True).astype(jnp.int32)
    groups = ITEMS // SLOTS
    slot_of = item_ids % groups * SLOTS + item_ids // groups
    tile_map = jnp.zeros((ITEMS,), jnp.int32).at[ordering].set(slot_of.astype(jnp.int32))
    return (steps, tile_map)


def draw_trunc_steps(key, part):
    return chain_plan(key)[0]


def draw_tile_map(key, part):
    return chain_plan(key)[1]


def with_ends(result, own_key, low, top_value):
    longest = result.shape.index(max(result.shape))
    spots = []
    for shift in (0, 1):
        where = [jax.random.randint(jax.random.fold_in(own_key, axis), (), 0, length) for axis, length in enumerate(result.shape)]
        where[longest] = (where[longest] + shift) % result.shape[longest]
        spots.append(tuple(where))
    return result.at[spots[0]].set(low).at[spots[1]].set(top_value)


def block_scale(rng, extent, cuts, low, high):
    def one(dim, parts):
        draws = jax.random.uniform(jax.random.fold_in(jax.random.fold_in(rng, 6), dim), (parts,), jnp.float32, low / len(cuts), high / len(cuts))
        return jnp.repeat(jnp.exp(draws), extent[dim] // parts).reshape((-1,) + (1,) * (len(extent) - dim - 1))

    level = one(*cuts[0])
    for cut in cuts[1:]:
        level = level * one(*cut)
    return level


def bell_draw(stream_key, dims, scale, reach, cuts=(), held_as=jnp.bfloat16):
    drawn = scale * jax.random.normal(stream_key, dims, jnp.float32)
    if cuts:
        drawn = drawn * block_scale(stream_key, dims, cuts, -0.22, 0.18)
    return jnp.clip(drawn, -reach, reach).astype(held_as)


def setup_inputs(seed: int = 0) -> dict:
    key_of = jax.random.split(jax.random.key(seed), 10)
    return {
        "latents": bell_draw(key_of[0], (ITEMS, ROWS, C), 1.0, 6.0, ((0, 16), (1, 8))),
        "cotangent": bell_draw(key_of[1], (ITEMS, ROWS, C), 1.0, 6.0, ((0, 16), (1, 8))),
        "trunc_steps": draw_trunc_steps(jax.random.fold_in(key_of[9], 71), 0),
        "timesteps": with_ends(jax.random.randint(key_of[3], (ITEMS,), 100, 901), jax.random.fold_in(key_of[3], 1), 100, 900).astype(jnp.int32),
        "tile_map": draw_tile_map(jax.random.fold_in(key_of[9], 71), 0),
        "gain": jnp.clip(1.0 + 0.1 * jax.random.normal(key_of[5], (C,), jnp.float32), 0.5, 1.5),
        "w_value": bell_draw(key_of[6], (C, FI), C ** -0.5, 0.25, ((1, 8),)),
        "w_gate": bell_draw(key_of[7], (C, FI), C ** -0.5, 0.25, ((1, 8),)),
        "w_out": bell_draw(key_of[8], (C, FI), FI ** -0.5, 0.125, ((1, 8),)),
    }


eps = 1e-05

def alpha_bars():
    betas = jnp.linspace(0.00085 ** 0.5, 0.012 ** 0.5, 1000, dtype=jnp.float32) ** 2
    return jnp.exp(jnp.cumsum(jnp.log1p(-betas)))

def gelu_parts(inputs):
    cdf = 0.5 * (1.0 + lax.erf(inputs * 0.7071067811865476))
    density = jnp.exp(-0.5 * inputs * inputs) * 0.3989422804014327
    return (inputs * cdf, cdf + inputs * density)

def item_backward(normed, grad_tile, w_value, w_gate, w_out):
    values_proj = jnp.dot(normed, w_value, preferred_element_type=jnp.float32)
    gate_proj = jnp.dot(normed, w_gate, preferred_element_type=jnp.float32)
    gelu_gate, gelu_slope = gelu_parts(gate_proj)
    hidden = (values_proj * gelu_gate).astype(jnp.bfloat16)
    d_hidden = jnp.dot(grad_tile, w_out, preferred_element_type=jnp.float32)
    d_value = (d_hidden * gelu_gate).astype(jnp.bfloat16)
    d_gate = (d_hidden * values_proj * gelu_slope).astype(jnp.bfloat16)
    first_dims = (((0,), (0,)), ((), ()))
    last_dims = (((1,), (1,)), ((), ()))
    grad_wv = lax.dot_general(normed, d_value, first_dims, preferred_element_type=jnp.float32)
    grad_wg = lax.dot_general(normed, d_gate, first_dims, preferred_element_type=jnp.float32)
    grad_wo = lax.dot_general(grad_tile, hidden, first_dims, preferred_element_type=jnp.float32)
    d_normed = lax.dot_general(d_value, w_value, last_dims, preferred_element_type=jnp.float32)
    d_normed = d_normed + lax.dot_general(d_gate, w_gate, last_dims, preferred_element_type=jnp.float32)
    return (grad_wv, grad_wg, grad_wo, d_normed)

def reference(latents, cotangent, trunc_steps, timesteps, tile_map, gain, w_value, w_gate, w_out):
    total = latents.shape[0]
    item_ids = jnp.arange(total, dtype=jnp.int32)
    live = item_ids % SLOTS < jnp.repeat(trunc_steps, SLOTS) - 29
    noise_scale = jnp.sqrt(1.0 - alpha_bars()[timesteps])
    width = latents.shape[2]
    inner = w_value.shape[1]

    def one_item(carry, inputs):
        tile, cot_tile, item_scale, is_live = inputs
        x_float = tile.astype(jnp.float32)
        row_mean = lax.optimization_barrier(jnp.mean(x_float, axis=-1, keepdims=True))
        centred = x_float - row_mean
        row_var = lax.optimization_barrier(jnp.mean(centred * centred, axis=-1, keepdims=True))
        inv_std = lax.rsqrt(row_var + eps)
        x_hat = centred * inv_std
        normed = (x_hat * gain).astype(jnp.bfloat16)
        grad_tile = (cot_tile.astype(jnp.float32) * item_scale).astype(jnp.bfloat16)

        def run(unused):
            grad_wv, grad_wg, grad_wo, d_normed = item_backward(normed, grad_tile, w_value, w_gate, w_out)
            d_hat = d_normed * gain
            input_grad = grad_tile.astype(jnp.float32) + inv_std * (d_hat - lax.optimization_barrier(jnp.mean(d_hat, axis=-1, keepdims=True)) - x_hat * lax.optimization_barrier(jnp.mean(d_hat * x_hat, axis=-1, keepdims=True)))
            gain_part = lax.optimization_barrier(jnp.sum(d_normed * x_hat, axis=0))
            return (grad_wv, grad_wg, grad_wo, gain_part, input_grad.astype(jnp.bfloat16))

        def skip(unused):
            zero_w = jnp.zeros((width, inner), jnp.float32)
            return (zero_w, zero_w, zero_w, jnp.zeros((width,), jnp.float32), jnp.zeros(tile.shape, jnp.bfloat16))
        grad_wv, grad_wg, grad_wo, gain_part, input_grad = lax.cond(is_live, run, skip, None)
        carry = (carry[0] + grad_wv, carry[1] + grad_wg, carry[2] + grad_wo, carry[3] + gain_part)
        return (carry, input_grad)
    zero_w = jnp.zeros((width, inner), jnp.float32)
    init = (zero_w, zero_w, zero_w, jnp.zeros((width,), jnp.float32))
    sums, input_grads = lax.scan(one_item, init, (latents, cotangent, noise_scale, live))
    placed_grad = jnp.zeros(latents.shape, jnp.bfloat16).at[tile_map.astype(jnp.int32)].set(input_grads)
    return (placed_grad, sums[0], sums[1], sums[2], sums[3])
```

```python
import functools

import jax
import jax.numpy as jnp
import numpy as np
from jax import lax
from jax.experimental import pallas as pl
from jax.experimental.pallas import tpu as pltpu
from jax.sharding import Mesh
from jax.sharding import PartitionSpec as P

AXES = ("dp_0", "dp_1", "dp_2", "tensor_0", "tensor_1")
TENSOR = ("tensor_0", "tensor_1")
DP = ("dp_0", "dp_1", "dp_2")

C = 640
S = 11
W = 32
G = 16
HL = 320
HP = 384
F = 2 * HP
BLK = 48
EPS = 1e-05
MESH_ID = pl.DeviceIdType.MESH
BF = jnp.bfloat16
F32 = jnp.float32
TN = (((0,), (0,)), ((), ()))
NT = (((1,), (1,)), ((), ()))
SIZES = (5, 6, 7, 8, 11)


def scale_table():
    betas = np.linspace(0.00085**0.5, 0.012**0.5, 1000, dtype=np.float64) ** 2
    return np.sqrt(1.0 - np.exp(np.cumsum(np.log1p(-betas)))).astype(np.float32)


def iota(shape, dim):
    return lax.broadcasted_iota(jnp.int32, shape, dim)


def one_hot(rows, columns):
    return jnp.where(rows == columns, 1.0, 0.0).astype(BF)


def body(
    n,
    table, times, steps, code, gain, x, cot, wv, wg, wo,
    out, gwv, gwg, gwo, ggain,
    xg, onehot, z1, r1, z2, r2, xhat, inv, wcat, agn, agg, vg, dh, act, part, pin, own, tr, dw,
    cs, cr, xs, xr, gy, gc, gx,
    s1s, s1r, s2s, s2r, ags, agr, rss, rsr, cds, cdr, xds, xdr, wds, wdr, gys, gyr, gcs, gcr, gxs, gxr,
):
    rp = -(-4 * n // 16) * 16
    rows = W * n
    ax, az, ak = (lax.axis_index(a) for a in DP)
    ay, al = (lax.axis_index(a) for a in TENSOR)
    p = ax * 8 + az * 2 + ak
    e = (ax * 4 + az) * 2 + al

    def dp_dev(j):
        return {"dp_0": j // 8, "dp_1": lax.rem(j // 2, 4), "dp_2": lax.rem(j, 2)}

    def xz_dev(j):
        return {"dp_0": j // 8, "dp_1": lax.rem(j // 2, 4), "tensor_1": lax.rem(j, 2)}

    def y_dev(step):
        return {"tensor_0": lax.rem(ay + step, 4)}

    core = {"dp_2": 1 - ak}
    pair = {"tensor_1": 1 - al}

    def rcopy(src, dst, send, recv, dev):
        return pltpu.make_async_remote_copy(
            src_ref=src, dst_ref=dst, send_sem=send, recv_sem=recv,
            device_id=dev, device_id_type=MESH_ID,
        )

    barrier = pltpu.get_barrier_semaphore()

    def greet(dev):
        pl.semaphore_signal(barrier, inc=1, device_id=dev, device_id_type=MESH_ID)

    @pl.loop(1, 16)
    def _(d):
        greet(dp_dev(lax.rem(p + d, 16)))

    @pl.loop(1, 16)
    def _(d):
        greet(xz_dev(lax.rem(e + d, 16)))

    for step in (1, 2, 3):
        greet(y_dev(step))

    for i in range(S):
        scale = table[times[p * S + i]]
        scale = jnp.where(i < steps[p] - 29, scale, 0.0)
        xg[i * W : (i + 1) * W, :] = x[i]
        xg[(S + i) * W : (S + i + 1) * W, :] = (cot[i].astype(F32) * scale).astype(BF)

    q = iota((BLK, 1), 0)
    arr = jnp.where(q >= 2 * S, 1, 0)
    src = arr * (S * W) + ((q - 2 * S * arr) >> 1) * W + (q & 1)
    src = jnp.where(q >= 4 * S, -4096, src)
    lane = iota((BLK, 2 * S * W), 1)
    for j in range(G):
        onehot[j * BLK : (j + 1) * BLK, : 2 * S * W] = one_hot(src + 2 * j, lane)
    z1[...] = jnp.dot(
        onehot[:, : 2 * S * W], xg[...], preferred_element_type=F32
    ).astype(BF).reshape(G, BLK, C)

    zero = jnp.zeros((C, HP - 256), BF)
    for m, w in enumerate((wv, wg, wo)):
        wcat[:, m * F + 256 : m * F + HP] = zero
        wcat[:, m * F : m * F + HL] = w[...]

    pl.semaphore_wait(barrier, 33)

    def w_copy(m, stage):
        at = pl.ds(pl.multiple_of(ak * HL, HL), HL)
        if stage == 0:
            return rcopy(
                wcat.at[at, pl.ds(m * F, HP)], wcat.at[at, pl.ds(m * F + HP, HP)],
                wds.at[m], wdr.at[m], pair,
            )
        part_ref = wcat.at[at, pl.ds(m * F + HP, HP)]
        return rcopy(part_ref, part_ref, wds.at[3 + m], wdr.at[3 + m], core)

    def spread(j):
        return rcopy(z1.at[j], r1.at[p], s1s.at[j], s1r.at[p], dp_dev(j))

    def spread_in(j):
        return rcopy(z1.at[j], r1.at[j], s1s.at[j], s1r.at[j], dp_dev(j))

    @pl.loop(1, 16)
    def _(d):
        spread(lax.rem(p + d, 16)).start()

    for m in range(3):
        w_copy(m, 0).start()
    r1[p] = z1[p]

    q = iota((rp, 1), 0)
    arr = jnp.where(q >= 2 * n, 1, 0)
    tail = arr * 2 + (q & 1)
    slot = (q - 2 * n * arr) >> 1
    for j in range(G):
        want = jnp.where(q >= 4 * n, -7, (slot + j * S) * 4 + tail)
        onehot[j * rp : (j + 1) * rp, :] = one_hot(want, code[...])

    @pl.loop(1, 16)
    def _(d):
        spread_in(lax.rem(p + d, 16)).wait_recv()

    z2[...] = jnp.dot(
        onehot[: G * rp, :], r1[...].reshape(G * BLK, C), preferred_element_type=F32
    ).astype(BF).reshape(G, rp, C)

    def deliver(j):
        return rcopy(z2.at[j], r2.at[p], s2s.at[j], s2r.at[p], dp_dev(j))

    def deliver_in(j):
        return rcopy(z2.at[j], r2.at[j], s2s.at[j], s2r.at[j], dp_dev(j))

    @pl.loop(1, 16)
    def _(d):
        deliver(lax.rem(p + d, 16)).start()

    r2[p] = z2[p]

    q = iota((rows, 1), 0)
    w = q & (W - 1)
    src = (w >> 1) * rp + (q >> 5) * 2 + (w & 1)
    lane = iota((rows, G * rp), 1)
    onehot[:rows, : G * rp] = one_hot(src, lane)
    onehot[rows : 2 * rows, : G * rp] = one_hot(src + 2 * n, lane)

    for m in range(3):
        w_copy(m, 0).wait_recv()
        w_copy(m, 1).start()

    @pl.loop(1, 16)
    def _(d):
        deliver_in(lax.rem(p + d, 16)).wait_recv()

    got = r2[...].reshape(G * rp, C)
    xhat[...] = jnp.dot(onehot[:rows, : G * rp], got, preferred_element_type=F32)
    agg[ay] = jnp.dot(
        onehot[rows : 2 * rows, : G * rp], got, preferred_element_type=F32
    ).astype(BF)

    @pl.loop(0, n)
    def _(k):
        at = pl.ds(pl.multiple_of(k * W, W), W)
        tile = xhat[at, :]
        centred = tile - jnp.mean(tile, axis=-1, keepdims=True)
        std = lax.rsqrt(jnp.mean(centred * centred, axis=-1, keepdims=True) + EPS)
        hat = centred * std
        xhat[at, :] = hat
        inv[at, :] = std
        agn[ay, at, :] = (hat * gain[...]).astype(BF)

    left, right, far = (lax.rem(ay + s, 4) for s in (3, 1, 2))
    bufs = (agn, agg)

    def gather(a, step):
        k = 0 if step == 1 else 1
        return rcopy(bufs[a].at[ay], bufs[a].at[ay], ags.at[2 * k + a], agr.at[2 * k + a], y_dev(step))

    def gather_in(a, step):
        k = 0 if step == 1 else 1
        frm = left if step == 1 else right
        return rcopy(bufs[a].at[frm], bufs[a].at[frm], ags.at[2 * k + a], agr.at[2 * k + a], y_dev(step))

    def pass_on(a):
        frm, step = (left, 1) if a == 0 else (right, 3)
        return rcopy(bufs[a].at[frm], bufs[a].at[frm], ags.at[4 + a], agr.at[4 + a], y_dev(step))

    def pass_in(a):
        return rcopy(bufs[a].at[far], bufs[a].at[far], ags.at[4 + a], agr.at[4 + a], y_dev(1))

    gather(0, 1).start()
    gather(1, 3).start()
    gather(1, 1).start()
    gather(0, 3).start()

    for m in range(3):
        w_copy(m, 1).wait_recv()

    def compute(frm):
        vg[...] = jnp.dot(agn[frm], wcat[:, : 2 * F], preferred_element_type=F32)
        dh[...] = jnp.dot(agg[frm], wcat[:, 2 * F :], preferred_element_type=F32)

        @pl.loop(0, rows // 16)
        def _(b):
            at = pl.ds(pl.multiple_of(b * 16, 16), 16)
            to = pl.ds(pl.multiple_of(frm * rows + b * 16, 16), 16)
            for u in range(F // 256):
                lo, hi = u * 256, (u + 1) * 256
                val = vg[at, lo:hi]
                gate = vg[at, F + lo : F + hi]
                dhid = dh[at, lo:hi]
                cdf = 0.5 * (1.0 + lax.erf(gate * 0.7071067811865476))
                dens = jnp.exp(-0.5 * gate * gate) * 0.3989422804014327
                gel = gate * cdf
                act[to, lo:hi] = (dhid * gel).astype(BF)
                act[to, F + lo : F + hi] = (dhid * val * (cdf + gate * dens)).astype(BF)
                act[to, 2 * F + lo : 2 * F + hi] = (val * gel).astype(BF)

        here = pl.ds(pl.multiple_of(frm * rows, rows), rows)
        return lax.dot_general(
            act[here, : 2 * F], wcat[:, : 2 * F], NT, preferred_element_type=F32
        )

    def give(step):
        return rcopy(part.at[step - 1], pin.at[step - 1], rss.at[step - 1], rsr.at[step - 1], y_dev(step))

    own[...] = compute(ay)
    gather_in(0, 1).wait_recv()
    pass_on(0).start()
    gather_in(1, 3).wait_recv()
    pass_on(1).start()
    gather_in(1, 1).wait_recv()
    part[2] = compute(left).astype(BF)
    give(3).start()
    gather_in(0, 3).wait_recv()
    part[0] = compute(right).astype(BF)
    give(1).start()
    pass_in(0).wait_recv()
    pass_in(1).wait_recv()
    part[1] = compute(far).astype(BF)
    give(2).start()

    tr[...] = agn[...].reshape(4 * rows, C).T

    @pl.loop(0, 2 * F // HP)
    def _(b):
        at = pl.ds(pl.multiple_of(b * HP, HP), HP)
        dw[:, at] = jnp.dot(tr[...], act[:, at], preferred_element_type=F32)

    tr[...] = agg[...].reshape(4 * rows, C).T

    @pl.loop(2 * F // HP, 3 * F // HP)
    def _(b):
        at = pl.ds(pl.multiple_of(b * HP, HP), HP)
        dw[:, at] = jnp.dot(tr[...], act[:, at], preferred_element_type=F32)

    @pl.loop(0, 8)
    def _(b):
        at = pl.ds(pl.multiple_of(40 * (2 * b + 1 - ak), 8), 40)
        cs[b] = dw[at, :].astype(BF)

    core_copy = rcopy(cs, cr, cds, cdr, core)
    core_copy.start()

    for step in (1, 2, 3):
        give(step).wait_recv()

    gacc = jnp.zeros((1, C), F32)

    def finish(k, acc):
        at = pl.ds(pl.multiple_of(k * W, W), W)
        dn = own[at, :] + pin[0, at, :].astype(F32)
        dn = dn + pin[1, at, :].astype(F32)
        dn = dn + pin[2, at, :].astype(F32)
        hat = xhat[at, :]
        dhat = dn * gain[...]
        grad = agg[ay, at, :].astype(F32) + inv[at, :] * (
            dhat
            - jnp.mean(dhat, axis=-1, keepdims=True)
            - hat * jnp.mean(dhat * hat, axis=-1, keepdims=True)
        )
        out[k] = grad.astype(BF)
        return acc + jnp.sum(dn * hat, axis=0, keepdims=True)

    gacc = lax.fori_loop(0, n, finish, gacc)
    if n < S:
        out[n:] = jnp.zeros((S - n, W, C), BF)

    gy[ay] = gacc

    def gy_copy(step):
        return rcopy(gy.at[ay], gy.at[ay], gys.at[step - 1], gyr.at[ay], y_dev(step))

    def gy_in(step):
        frm = lax.rem(ay + step, 4)
        return rcopy(gy.at[frm], gy.at[frm], gys.at[step - 1], gyr.at[frm], y_dev(step))

    for step in (1, 2, 3):
        gy_copy(step).start()
    for step in (1, 2, 3):
        gy_in(step).wait_recv()
    gc[ak] = gy[0] + gy[1] + gy[2] + gy[3]
    gc_copy = rcopy(gc.at[ak], gc.at[ak], gcs.at[0], gcr.at[ak], core)
    gc_copy.start()

    core_copy.wait_recv()

    @pl.loop(0, 8)
    def _(b):
        at = pl.ds(pl.multiple_of(40 * (2 * b + ak), 8), 40)
        both = dw[at, :] + cr[b].astype(F32)
        for h in range(2):
            to = b * 2 + lax.rem(al + h, 2)
            for m in range(3):
                lo = m * F + h * HP
                xs[to, :, m * HP : (m + 1) * HP] = both[:, lo : lo + HP].astype(BF)

    def plane(j):
        return rcopy(xs.at[j], xr.at[e], xds.at[j], xdr.at[e], xz_dev(j))

    def plane_in(j):
        return rcopy(xs.at[j], xr.at[j], xds.at[j], xdr.at[j], xz_dev(j))

    @pl.loop(1, 16)
    def _(d):
        plane(lax.rem(e + d, 16)).start()

    xr[e] = xs[e]
    rcopy(gc.at[1 - ak], gc.at[1 - ak], gcs.at[0], gcr.at[1 - ak], core).wait_recv()
    gx[e] = gc[0] + gc[1]

    def gx_copy(j):
        return rcopy(gx.at[e], gx.at[e], gxs.at[j], gxr.at[e], xz_dev(j))

    def gx_in(j):
        return rcopy(gx.at[j], gx.at[j], gxs.at[j], gxr.at[j], xz_dev(j))

    @pl.loop(1, 16)
    def _(d):
        gx_copy(lax.rem(e + d, 16)).start()

    @pl.loop(1, 16)
    def _(d):
        gx_in(lax.rem(e + d, 16)).wait_recv()

    total = gx[0]
    for j in range(1, G):
        total = total + gx[j]
    ggain[...] = total

    @pl.loop(1, 16)
    def _(d):
        plane_in(lax.rem(e + d, 16)).wait_recv()

    for m, ref in enumerate((gwv, gwg, gwo)):
        lo = m * HP
        acc = xr[0, :, lo : lo + HP].astype(F32)
        for j in range(1, G):
            acc = acc + xr[j, :, lo : lo + HP].astype(F32)
        ref[...] = acc[:, :HL]

    @pl.loop(1, 16)
    def _(d):
        spread(lax.rem(p + d, 16)).wait_send()
        deliver(lax.rem(p + d, 16)).wait_send()
        plane(lax.rem(e + d, 16)).wait_send()
        gx_copy(lax.rem(e + d, 16)).wait_send()

    for m in range(3):
        w_copy(m, 0).wait_send()
        w_copy(m, 1).wait_send()
    for a in range(2):
        gather(a, 1).wait_send()
        gather(a, 3).wait_send()
        pass_on(a).wait_send()
    for step in (1, 2, 3):
        give(step).wait_send()
        gy_copy(step).wait_send()
    core_copy.wait_send()
    gc_copy.wait_send()


def call(n, index, table, times, steps, code, gain, x, cot, wv, wg, wo):
    rp = -(-4 * n // 16) * 16
    rows = W * n
    dma = pltpu.SemaphoreType.DMA
    vmem = pl.BlockSpec(memory_space=pltpu.VMEM)
    smem = pl.BlockSpec(memory_space=pltpu.SMEM)
    scratch = [
        ((2 * S * W, C), BF), ((768, 768), BF), ((G, BLK, C), BF), ((G, BLK, C), BF),
        ((G, rp, C), BF), ((G, rp, C), BF), ((rows, C), F32), ((rows, 1), F32),
        ((C, 3 * F), BF), ((4, rows, C), BF), ((4, rows, C), BF), ((rows, 2 * F), F32),
        ((rows, F), F32), ((4 * rows, 3 * F), BF), ((3, rows, C), BF), ((3, rows, C), BF),
        ((rows, C), F32), ((C, 4 * rows), BF), ((C, 3 * F), F32),
        ((8, 40, 3 * F), BF), ((8, 40, 3 * F), BF), ((G, 40, 3 * HP), BF), ((G, 40, 3 * HP), BF),
        ((4, 1, C), F32), ((2, 1, C), F32), ((G, 1, C), F32),
    ]
    sems = [
        dma((16,)), dma((16,)), dma((16,)), dma((16,)), dma((6,)), dma((6,)), dma((3,)), dma((3,)),
        dma, dma, dma((16,)), dma((16,)), dma((6,)), dma((6,)), dma((3,)), dma((4,)),
        dma((1,)), dma((2,)), dma((16,)), dma((16,)),
    ]
    return pl.pallas_call(
        functools.partial(body, n),
        out_shape=(
            jax.ShapeDtypeStruct((S, W, C), BF),
            jax.ShapeDtypeStruct((40, HL), F32),
            jax.ShapeDtypeStruct((40, HL), F32),
            jax.ShapeDtypeStruct((40, HL), F32),
            jax.ShapeDtypeStruct((1, C), F32),
        ),
        in_specs=[smem, smem, smem] + [vmem] * 7,
        out_specs=(vmem,) * 5,
        scratch_shapes=[pltpu.VMEM(s, t) for s, t in scratch] + sems,
        compiler_params=pltpu.CompilerParams(
            collective_id=index, has_side_effects=True, vmem_limit_bytes=62 * 1024 * 1024
        ),
        name="chain_backward",
    )(table, times, steps, code, gain, x, cot, wv, wg, wo)


def per_device(latents, cotangent, trunc_steps, timesteps, tile_map, gain, w_value, w_gate, w_out):
    tail = (2 * jnp.arange(2)[:, None, None] + jnp.arange(2)[None, None, :]).astype(jnp.int32)
    code = tile_map.reshape(G, 1, S, 1) * 4 + tail[None]
    code = jnp.pad(code.reshape(G, 4 * S), ((0, 0), (0, BLK - 4 * S)), constant_values=-1)
    live = jnp.sum(trunc_steps - 29)
    need = (live + G - 1) // G
    args = (
        jnp.asarray(scale_table()), timesteps, trunc_steps, code.reshape(1, G * BLK),
        gain.reshape(1, C), latents, cotangent, w_value, w_gate, w_out,
    )
    which = jnp.sum((need > jnp.asarray(SIZES[:-1], jnp.int32)).astype(jnp.int32))
    branches = [functools.partial(call, n, i) for i, n in enumerate(SIZES)]
    placed, gwv, gwg, gwo, ggain = lax.switch(which, branches, *args)
    return (placed, gwv, gwg, gwo, ggain.reshape(C))


def solution(mesh):
    split = Mesh(mesh.devices.reshape(2, 4, 2, 4, 2), AXES)
    weights = P(None, TENSOR)
    in_specs = (P(DP, TENSOR, None),) * 2 + (P(),) * 4 + (weights,) * 3
    out_specs = (P(DP, TENSOR, None), P(DP, TENSOR), P(DP, TENSOR), P(DP, TENSOR), P())
    return jax.shard_map(
        per_device, mesh=split, in_specs=in_specs, out_specs=out_specs, check_vma=False
    )
```

```python
import functools

import jax
import jax.numpy as jnp
import numpy as np
from jax import lax
from jax.experimental import pallas as pl
from jax.experimental.pallas import tpu as pltpu
from jax.sharding import Mesh
from jax.sharding import PartitionSpec as P

AXES = ("dp_0", "dp_1", "dp_2", "tensor_0", "tensor_1")
TENSOR = ("tensor_0", "tensor_1")
DP = ("dp_0", "dp_1", "dp_2")

C = 640
S = 11
W = 32
G = 16
HL = 320
HP = 384
F = 2 * HP
BLK = 48
EPS = 1e-05
MESH_ID = pl.DeviceIdType.MESH
BF = jnp.bfloat16
F32 = jnp.float32
TN = (((0,), (0,)), ((), ()))
NT = (((1,), (1,)), ((), ()))
SIZES = (6, 7, 8, 11)
STOP = 99


def scale_table():
    betas = np.linspace(0.00085**0.5, 0.012**0.5, 1000, dtype=np.float64) ** 2
    return np.sqrt(1.0 - np.exp(np.cumsum(np.log1p(-betas)))).astype(np.float32)


def iota(shape, dim):
    return lax.broadcasted_iota(jnp.int32, shape, dim)


def one_hot(rows, columns):
    return jnp.where(rows == columns, 1.0, 0.0).astype(BF)


def body(
    n,
    table, times, steps, tmap, gain, x, cot, wv, wg, wo,
    out, gwv, gwg, gwo, ggain,
    xg, cots, code, onehot, z1, r1, z2, r2, xhat, inv, wcat, agn, agg, vg, dh, act, part, pin, own, tr, dw,
    cs, cr, xs, xr, gy, gc, gx, lds,
    s1s, s1r, s2s, s2r, ags, agr, rss, rsr, cds, cdr, xds, xdr, wds, wdr, gys, gyr, gcs, gcr, gxs, gxr,
):
    rp = -(-4 * n // 16) * 16
    rows = W * n
    ax, az, ak = (lax.axis_index(a) for a in DP)
    ay, al = (lax.axis_index(a) for a in TENSOR)
    p = ax * 8 + az * 2 + ak
    e = (ax * 4 + az) * 2 + al

    def dp_dev(j):
        return {"dp_0": j // 8, "dp_1": lax.rem(j // 2, 4), "dp_2": lax.rem(j, 2)}

    def xz_dev(j):
        return {"dp_0": j // 8, "dp_1": lax.rem(j // 2, 4), "tensor_1": lax.rem(j, 2)}

    def y_dev(step):
        return {"tensor_0": lax.rem(ay + step, 4)}

    core = {"dp_2": 1 - ak}

    def rcopy(src, dst, send, recv, dev):
        return pltpu.make_async_remote_copy(
            src_ref=src, dst_ref=dst, send_sem=send, recv_sem=recv,
            device_id=dev, device_id_type=MESH_ID,
        )

    loads = [pltpu.make_async_copy(x, xg.at[:S], lds.at[0]), pltpu.make_async_copy(cot, cots, lds.at[1])]
    for m, w in enumerate((wv, wg, wo)):
        loads.append(pltpu.make_async_copy(w, wcat.at[pl.ds(m * F, HL), :], lds.at[2 + m]))
    for load in loads:
        load.start()

    barrier = pltpu.get_barrier_semaphore()

    def greet(dev):
        pl.semaphore_signal(barrier, inc=1, device_id=dev, device_id_type=MESH_ID)

    @pl.loop(1, 16)
    def _(d):
        greet(dp_dev(lax.rem(p + d, 16)))
        greet(xz_dev(lax.rem(e + d, 16)))

    for step in (1, 2, 3):
        greet(y_dev(step))

    q = iota((BLK, 1), 0)
    arr = jnp.where(q >= 2 * S, 1, 0)
    src = arr * (S * W) + ((q - 2 * S * arr) >> 1) * W + (q & 1)
    src = jnp.where(q >= 4 * S, -4096, src)
    lane = iota((BLK, 2 * S * W), 1)

    @pl.loop(0, G)
    def _(j):
        at = pl.ds(pl.multiple_of(j * BLK, BLK), BLK)
        onehot[at, : 2 * S * W] = one_hot(src + 2 * j, lane)

    loads[0].wait()
    loads[1].wait()

    @pl.loop(0, S)
    def _(i):
        scale = table[times[p * S + i]]
        scale = jnp.where(i < steps[p] - 29, scale, 0.0)
        xg[S + i] = (cots[i].astype(F32) * scale).astype(BF)

    z1[...] = jnp.dot(
        onehot[:, : 2 * S * W], xg[...].reshape(2 * S * W, C), preferred_element_type=F32
    ).astype(BF).reshape(G, BLK, C)

    pl.semaphore_wait(barrier, 33)

    def w_copy(m, stage):
        half = pl.multiple_of(ak * (HL // 2), HL // 2)
        mine = wcat.at[pl.ds(m * F + half, HL // 2), :]
        theirs = wcat.at[pl.ds(m * F + HP + half, HL // 2), :]
        if stage == 0:
            to = lax.rem(2 * ax + al + 1 + 2 * ak, 4)
            dev = {"dp_0": to // 2, "tensor_1": lax.rem(to, 2)}
            return rcopy(mine, theirs, wds.at[m], wdr.at[m], dev)
        return rcopy(theirs, theirs, wds.at[3 + m], wdr.at[3 + m], core)

    def spread(j):
        return rcopy(z1.at[j], r1.at[p], s1s.at[j], s1r.at[p], dp_dev(j))

    def spread_in(j):
        return rcopy(z1.at[j], r1.at[j], s1s.at[j], s1r.at[j], dp_dev(j))

    @pl.loop(1, 16)
    def _(d):
        spread(lax.rem(p + d, 16)).start()

    r1[p] = z1[p]

    zero = jnp.zeros((HP - HL, C), BF)
    for m in range(6):
        wcat[m * HP + HL : (m + 1) * HP, :] = zero
    col = iota((1, G * BLK), 1)
    grp = (col * 1366) >> 16
    rest = col - BLK * grp
    arr = jnp.where(rest >= 2 * S, 1, 0)
    rest2 = rest - 2 * S * arr
    item = grp * S + (rest2 >> 1)
    pick = one_hot(iota((G * S, G * BLK), 0), item)
    slots = jnp.dot(tmap[...].astype(F32).astype(BF), pick, preferred_element_type=F32)
    codes = slots.astype(jnp.int32) * 4 + arr * 2 + (rest2 & 1)
    code[...] = jnp.where(rest >= 4 * S, -1, codes)

    q = iota((rp, 1), 0)
    arr = jnp.where(q >= 2 * n, 1, 0)
    tail = arr * 2 + (q & 1)
    slot = (q - 2 * n * arr) >> 1

    @pl.loop(0, G)
    def _(j):
        at = pl.ds(pl.multiple_of(j * rp, rp), rp)
        want = jnp.where(q >= 4 * n, -7, (slot + j * S) * 4 + tail)
        onehot[at, :] = one_hot(want, code[...])

    @pl.loop(1, 16)
    def _(d):
        spread_in(lax.rem(p + d, 16)).wait_recv()

    z2[...] = jnp.dot(
        onehot[: G * rp, :], r1[...].reshape(G * BLK, C), preferred_element_type=F32
    ).astype(BF).reshape(G, rp, C)

    def deliver(j):
        return rcopy(z2.at[j], r2.at[p], s2s.at[j], s2r.at[p], dp_dev(j))

    def deliver_in(j):
        return rcopy(z2.at[j], r2.at[j], s2s.at[j], s2r.at[j], dp_dev(j))

    @pl.loop(1, 16)
    def _(d):
        deliver(lax.rem(p + d, 16)).start()

    for m in range(3):
        loads[2 + m].wait()
        w_copy(m, 0).start()
    r2[p] = z2[p]

    q = iota((rows, 1), 0)
    w = q & (W - 1)
    src = (w >> 1) * rp + (q >> 5) * 2 + (w & 1)
    lane = iota((rows, G * rp), 1)
    onehot[:rows, : G * rp] = one_hot(src, lane)
    onehot[rows : 2 * rows, : G * rp] = one_hot(src + 2 * n, lane)

    @pl.loop(1, 16)
    def _(d):
        deliver_in(lax.rem(p + d, 16)).wait_recv()

    got = r2[...].reshape(G * rp, C)
    xhat[...] = jnp.dot(onehot[:rows, : G * rp], got, preferred_element_type=F32)
    agg[ay] = jnp.dot(
        onehot[rows : 2 * rows, : G * rp], got, preferred_element_type=F32
    ).astype(BF)

    @pl.loop(0, n)
    def _(k):
        at = pl.ds(pl.multiple_of(k * W, W), W)
        tile = xhat[at, :]
        centred = tile - jnp.mean(tile, axis=-1, keepdims=True)
        std = lax.rsqrt(jnp.mean(centred * centred, axis=-1, keepdims=True) + EPS)
        hat = centred * std
        xhat[at, :] = hat
        inv[at, :] = std
        agn[ay, at, :] = (hat * gain[...]).astype(BF)

    left, right, far = (lax.rem(ay + s, 4) for s in (3, 1, 2))
    bufs = (agn, agg)

    def gather(a, step):
        k = 0 if step == 1 else 1
        return rcopy(bufs[a].at[ay], bufs[a].at[ay], ags.at[2 * k + a], agr.at[2 * k + a], y_dev(step))

    def gather_in(a, step):
        k = 0 if step == 1 else 1
        frm = left if step == 1 else right
        return rcopy(bufs[a].at[frm], bufs[a].at[frm], ags.at[2 * k + a], agr.at[2 * k + a], y_dev(step))

    def pass_on(a):
        frm, step = (left, 1) if a == 0 else (right, 3)
        return rcopy(bufs[a].at[frm], bufs[a].at[frm], ags.at[4 + a], agr.at[4 + a], y_dev(step))

    def pass_in(a):
        return rcopy(bufs[a].at[far], bufs[a].at[far], ags.at[4 + a], agr.at[4 + a], y_dev(1))

    gather(0, 1).start()
    gather(1, 3).start()
    gather(1, 1).start()
    gather(0, 3).start()

    gather_in(0, 1).wait_recv()
    pass_on(0).start()
    gather_in(1, 3).wait_recv()
    pass_on(1).start()
    for m in range(3):
        w_copy(m, 0).wait_recv()
        w_copy(m, 1).start()
    for m in range(3):
        w_copy(m, 1).wait_recv()

    def compute(frm):
        vg[...] = lax.dot_general(
            agn[frm], wcat[: 2 * F, :], NT, preferred_element_type=F32
        )
        dh[...] = lax.dot_general(
            agg[frm], wcat[2 * F :, :], NT, preferred_element_type=F32
        )

        @pl.loop(0, rows // 16)
        def _(b):
            at = pl.ds(pl.multiple_of(b * 16, 16), 16)
            to = pl.ds(pl.multiple_of(frm * rows + b * 16, 16), 16)
            for u in range(F // 256):
                lo, hi = u * 256, (u + 1) * 256
                val = vg[at, lo:hi]
                gate = vg[at, F + lo : F + hi]
                dhid = dh[at, lo:hi]
                cdf = 0.5 * (1.0 + lax.erf(gate * 0.7071067811865476))
                dens = jnp.exp(-0.5 * gate * gate) * 0.3989422804014327
                gel = gate * cdf
                act[to, lo:hi] = (dhid * gel).astype(BF)
                act[to, F + lo : F + hi] = (dhid * val * (cdf + gate * dens)).astype(BF)
                act[to, 2 * F + lo : 2 * F + hi] = (val * gel).astype(BF)

        here = pl.ds(pl.multiple_of(frm * rows, rows), rows)
        dh[:, :C] = jnp.dot(act[here, : 2 * F], wcat[: 2 * F, :], preferred_element_type=F32)

    def give(step):
        return rcopy(part.at[step - 1], pin.at[step - 1], rss.at[step - 1], rsr.at[step - 1], y_dev(step))

    @pl.loop(0, 4)
    def _(t):
        @pl.when(t == 1)
        def _():
            gather_in(1, 1).wait_recv()

        @pl.when(t == 2)
        def _():
            gather_in(0, 3).wait_recv()

        @pl.when(t == 3)
        def _():
            pass_in(0).wait_recv()
            pass_in(1).wait_recv()
            give(1).start()
            give(3).start()

        step = lax.rem(3 * t, 4) - jnp.where(t >= 2, 1, 0) + jnp.where(t == 3, 2, 0)
        compute(lax.rem(ay + step, 4))

        @pl.when(t == 0)
        def _():
            own[...] = dh[:, :C]

        @pl.when(t > 0)
        def _():
            part[step - 1] = dh[:, :C].astype(BF)

    give(2).start()

    tr[0] = agn[...].reshape(4 * rows, C).T
    tr[1] = agg[...].reshape(4 * rows, C).T

    def core_copy(m):
        return rcopy(cs.at[m], cr.at[m], cds.at[m], cdr.at[m], core)

    for m in range(3):

        @pl.loop(2 * m, 2 * m + 2)
        def _(b):
            at = pl.ds(pl.multiple_of(b * HP, HP), HP)
            dw[:, at] = jnp.dot(tr[m // 2], act[:, at], preferred_element_type=F32)

        @pl.loop(0, 8)
        def _(b):
            at = pl.ds(pl.multiple_of(40 * (2 * b + 1 - ak), 8), 40)
            cs[m, b] = dw[at, m * F : (m + 1) * F].astype(BF)

        core_copy(m).start()

    def plane(m, j):
        return rcopy(xs.at[m, j], xr.at[m, e], xds.at[m, j], xdr.at[m, e], xz_dev(j))

    def plane_in(m, j):
        return rcopy(xs.at[m, j], xr.at[m, j], xds.at[m, j], xdr.at[m, j], xz_dev(j))

    for m in range(3):
        core_copy(m).wait_recv()

        @pl.loop(0, 8)
        def _(b):
            at = pl.ds(pl.multiple_of(40 * (2 * b + ak), 8), 40)
            both = dw[at, m * F : (m + 1) * F] + cr[m, b].astype(F32)
            xs[m, b * 2 + al] = both[:, :HP].astype(BF)
            xs[m, b * 2 + 1 - al] = both[:, HP:].astype(BF)

        @pl.loop(1, 16)
        def _(d):
            plane(m, lax.rem(e + d, 16)).start()

        xr[m, e] = xs[m, e]

    for step in (1, 2, 3):
        give(step).wait_recv()

    def finish(k, acc):
        at = pl.ds(pl.multiple_of(k * W, W), W)
        dn = own[at, :] + pin[0, at, :].astype(F32)
        dn = dn + pin[1, at, :].astype(F32)
        dn = dn + pin[2, at, :].astype(F32)
        hat = xhat[at, :]
        dhat = dn * gain[...]
        grad = agg[ay, at, :].astype(F32) + inv[at, :] * (
            dhat
            - jnp.mean(dhat, axis=-1, keepdims=True)
            - hat * jnp.mean(dhat * hat, axis=-1, keepdims=True)
        )
        out[k] = grad.astype(BF)
        return acc + jnp.sum(dn * hat, axis=0, keepdims=True)

    gy[ay] = lax.fori_loop(0, n, finish, jnp.zeros((1, C), F32))
    if n < S:
        out[n:] = jnp.zeros((S - n, W, C), BF)

    def gy_copy(step):
        return rcopy(gy.at[ay], gy.at[ay], gys.at[step - 1], gyr.at[ay], y_dev(step))

    def gy_in(step):
        frm = lax.rem(ay + step, 4)
        return rcopy(gy.at[frm], gy.at[frm], gys.at[step - 1], gyr.at[frm], y_dev(step))

    for step in (1, 2, 3):
        gy_copy(step).start()
    for step in (1, 2, 3):
        gy_in(step).wait_recv()
    gc[ak] = gy[0] + gy[1] + gy[2] + gy[3]
    gc_copy = rcopy(gc.at[ak], gc.at[ak], gcs.at[0], gcr.at[ak], core)
    gc_copy.start()
    rcopy(gc.at[1 - ak], gc.at[1 - ak], gcs.at[0], gcr.at[1 - ak], core).wait_recv()
    gx[e] = gc[0] + gc[1]

    def gx_copy(j):
        return rcopy(gx.at[e], gx.at[e], gxs.at[j], gxr.at[e], xz_dev(j))

    def gx_in(j):
        return rcopy(gx.at[j], gx.at[j], gxs.at[j], gxr.at[j], xz_dev(j))

    @pl.loop(1, 16)
    def _(d):
        gx_copy(lax.rem(e + d, 16)).start()

    for m, ref in enumerate((gwv, gwg, gwo)):

        @pl.loop(1, 16)
        def _(d):
            plane_in(m, lax.rem(e + d, 16)).wait_recv()

        acc = xr[m, 0].astype(F32)
        for j in range(1, G):
            acc = acc + xr[m, j].astype(F32)
        ref[...] = acc[:, :HL]

    @pl.loop(1, 16)
    def _(d):
        gx_in(lax.rem(e + d, 16)).wait_recv()

    total = gx[0]
    for j in range(1, G):
        total = total + gx[j]
    ggain[...] = total

    @pl.loop(1, 16)
    def _(d):
        spread(lax.rem(p + d, 16)).wait_send()
        deliver(lax.rem(p + d, 16)).wait_send()
        for m in range(3):
            plane(m, lax.rem(e + d, 16)).wait_send()
        gx_copy(lax.rem(e + d, 16)).wait_send()

    for m in range(3):
        w_copy(m, 0).wait_send()
        w_copy(m, 1).wait_send()
    for a in range(2):
        gather(a, 1).wait_send()
        gather(a, 3).wait_send()
        pass_on(a).wait_send()
    for step in (1, 2, 3):
        give(step).wait_send()
        gy_copy(step).wait_send()
    for m in range(3):
        core_copy(m).wait_send()
    gc_copy.wait_send()


def call(n, index, table, times, steps, tmap, gain, x, cot, wv, wg, wo):
    rp = -(-4 * n // 16) * 16
    rows = W * n
    dma = pltpu.SemaphoreType.DMA
    vmem = pl.BlockSpec(memory_space=pltpu.VMEM)
    smem = pl.BlockSpec(memory_space=pltpu.SMEM)
    scratch = [
        ((2 * S, W, C), BF), ((S, W, C), BF), ((1, G * BLK), jnp.int32), ((G * BLK, G * BLK), BF), ((G, BLK, C), BF), ((G, BLK, C), BF),
        ((G, rp, C), BF), ((G, rp, C), BF), ((rows, C), F32), ((rows, 1), F32),
        ((3 * F, C), BF), ((4, rows, C), BF), ((4, rows, C), BF), ((rows, 2 * F), F32),
        ((rows, F), F32), ((4 * rows, 3 * F), BF), ((3, rows, C), BF), ((3, rows, C), BF),
        ((rows, C), F32), ((2, C, 4 * rows), BF), ((C, 3 * F), F32),
        ((3, 8, 40, F), BF), ((3, 8, 40, F), BF), ((3, G, 40, HP), BF), ((3, G, 40, HP), BF),
        ((4, 1, C), F32), ((2, 1, C), F32), ((G, 1, C), F32),
    ]
    hbm = pl.BlockSpec(memory_space=pl.ANY)
    sems = [
        dma((5,)),
        dma((16,)), dma((16,)), dma((16,)), dma((16,)), dma((6,)), dma((6,)), dma((3,)), dma((3,)),
        dma((3,)), dma((3,)), dma((3, 16)), dma((3, 16)), dma((6,)), dma((6,)), dma((3,)), dma((4,)),
        dma((1,)), dma((2,)), dma((16,)), dma((16,)),
    ]
    return pl.pallas_call(
        functools.partial(body, n),
        out_shape=(
            jax.ShapeDtypeStruct((S, W, C), BF),
            jax.ShapeDtypeStruct((40, HL), F32),
            jax.ShapeDtypeStruct((40, HL), F32),
            jax.ShapeDtypeStruct((40, HL), F32),
            jax.ShapeDtypeStruct((1, C), F32),
        ),
        in_specs=[smem] * 3 + [vmem] * 2 + [hbm] * 5,
        out_specs=(vmem,) * 5,
        scratch_shapes=[pltpu.VMEM(s, t) for s, t in scratch] + sems,
        compiler_params=pltpu.CompilerParams(
            collective_id=index, has_side_effects=True, vmem_limit_bytes=62 * 1024 * 1024
        ),
        name="chain_backward",
    )(table, times, steps, tmap, gain, x, cot, wv, wg, wo)


def per_device(latents, cotangent, trunc_steps, timesteps, tile_map, gain, w_value, w_gate, w_out):
    live = jnp.sum(trunc_steps - 29, keepdims=True)
    args = (
        jnp.asarray(scale_table()), timesteps, trunc_steps, tile_map.reshape(1, G * S),
        gain.reshape(1, C), latents, cotangent, w_value.T, w_gate.T, w_out.T,
    )
    which = sum((live > G * n).astype(jnp.int32) for n in SIZES[:-1])
    branches = [functools.partial(call, n, i) for i, n in enumerate(SIZES)]
    placed, gwv, gwg, gwo, ggain = lax.switch(which.reshape(()), branches, *args)
    return (placed, gwv, gwg, gwo, ggain.reshape(C))


def solution(mesh):
    split = Mesh(mesh.devices.reshape(2, 4, 2, 4, 2), AXES)
    weights = P(None, TENSOR)
    in_specs = (P(DP, TENSOR, None),) * 2 + (P(),) * 4 + (weights,) * 3
    out_specs = (P(DP, TENSOR, None), P(DP, TENSOR), P(DP, TENSOR), P(DP, TENSOR), P())
    return jax.shard_map(
        per_device, mesh=split, in_specs=in_specs, out_specs=out_specs, check_vma=False
    )
```
